128 devices in a mesh: part: 1, data: 64 (over z, y, x), model: 2 (over core).
Axes of the slice: x: 4, y: 4, z: 4, core: 2. Of those that a mesh axis runs over, the one named last changes fastest.
Arguments:
- x: bfloat16 [2, 64, 1024, 1024], P(None, ('part', 'data'), 'model')
- lengths: int32 [2, 64], P(None, ('part', 'data'))
- norm_gain: bfloat16 [2, 1024], P(None, 'data')
- w_in: bfloat16 [2, 1024, 9216], P(None, 'data', 'model')
- w_kv: bfloat16 [2, 1024, 128], P(None, 'data')
- w_out: bfloat16 [2, 5120, 1024], P(None, 'model', 'data')
Outputs:
- output: bfloat16 [2, 64, 1024, 1024], P(None, ('part', 'data'), 'model')
All inputs are finite; a program needn't handle non-finite values.
Results may differ from the reference program's by a relative error of at most 0.0146278.
Values are sent between devices in bfloat16 or wider.
A program may use at most 1 GiB of HBM per device.

```python
import math
import jax
import jax.numpy as jnp
from jax import lax

N_MICRO = 2
N_LAYERS = 2
N_SEQS = 64
SEQ_LEN = 1024
D_MODEL = 1024
N_HEADS = 16
HEAD_DIM = 64
D_FF = 4096
MODEL_SHARDS = 2
FF_HEAD = D_FF // N_HEADS
UNIT_IN = HEAD_DIM + 2 * FF_HEAD
UNIT_OUT = HEAD_DIM + FF_HEAD
SHARD_ROWS = (N_HEADS // MODEL_SHARDS) * UNIT_OUT
NORM_EPS = 1e-6
NEG_BIG = -1e30
Q_GAIN = math.sqrt(max(math.log(SEQ_LEN / 8.0), 1.0))


def setup_inputs(seed: int = 0, part: int = 0) -> dict:
    part_keys = jax.random.split(jax.random.fold_in(jax.random.key(seed), part), 2)
    shared_keys = jax.random.split(jax.random.key(seed + 1), 4)
    x_act = jax.random.normal(part_keys[0], (N_MICRO, N_SEQS, SEQ_LEN, D_MODEL), jnp.float32)
    seq_lens = jax.random.randint(part_keys[1], (N_MICRO, N_SEQS), SEQ_LEN // 4, SEQ_LEN + 1)
    seq_lens = seq_lens.at[0, 0].set(SEQ_LEN).at[1, 0].set(SEQ_LEN // 4)
    gain_vals = jax.random.uniform(shared_keys[0], (N_LAYERS, D_MODEL), jnp.float32, 0.5, 1.5)
    col_scale = jnp.concatenate([jnp.full((HEAD_DIM,), Q_GAIN, jnp.float32), jnp.ones((2 * FF_HEAD,), jnp.float32)]) * (D_MODEL ** -0.5)
    w_in_vals = jax.random.normal(shared_keys[1], (N_LAYERS, D_MODEL, N_HEADS, UNIT_IN), jnp.float32) * col_scale
    w_kv_vals = jax.random.normal(shared_keys[2], (N_LAYERS, D_MODEL, 2 * HEAD_DIM), jnp.float32) * (D_MODEL ** -0.5)
    row_scale = jnp.concatenate([jnp.full((HEAD_DIM,), (N_HEADS * HEAD_DIM) ** -0.5, jnp.float32), jnp.full((FF_HEAD,), D_FF ** -0.5, jnp.float32)])
    w_out_vals = jax.random.normal(shared_keys[3], (N_LAYERS, N_HEADS, UNIT_OUT, D_MODEL), jnp.float32) * row_scale[:, None]
    return {
        "x": x_act.astype(jnp.bfloat16),
        "lengths": seq_lens.astype(jnp.int32),
        "norm_gain": gain_vals.astype(jnp.bfloat16),
        "w_in": w_in_vals.reshape(N_LAYERS, D_MODEL, N_HEADS * UNIT_IN).astype(jnp.bfloat16),
        "w_kv": w_kv_vals.astype(jnp.bfloat16),
        "w_out": w_out_vals.reshape(N_LAYERS, N_HEADS * UNIT_OUT, D_MODEL).astype(jnp.bfloat16),
    }


def layer_one_seq(x_seq, seq_len, gain_vec, w_in_l, w_kv_l, w_out_l):
    x_f32 = x_seq.astype(jnp.float32)
    centered = x_f32 - jnp.mean(x_f32, axis=-1, keepdims=True)
    variance = jnp.mean(centered * centered, axis=-1, keepdims=True)
    h_act = (centered * lax.rsqrt(variance + NORM_EPS) * gain_vec.astype(jnp.float32)).astype(jnp.bfloat16)
    projected = jnp.dot(h_act, w_in_l, preferred_element_type=jnp.float32).astype(jnp.bfloat16)
    projected = projected.reshape(SEQ_LEN, N_HEADS, UNIT_IN)
    q_heads = projected[:, :, :HEAD_DIM]
    gate_act = projected[:, :, HEAD_DIM:HEAD_DIM + FF_HEAD]
    up_act = projected[:, :, HEAD_DIM + FF_HEAD:]
    kv_act = jnp.dot(h_act, w_kv_l, preferred_element_type=jnp.float32).astype(jnp.bfloat16)
    k_act = kv_act[:, :HEAD_DIM]
    v_act = kv_act[:, HEAD_DIM:]
    scores = jnp.einsum("qhc,kc->hqk", q_heads.astype(jnp.float32), k_act.astype(jnp.float32)) * (1.0 / math.sqrt(HEAD_DIM))
    positions = jnp.arange(SEQ_LEN)
    allowed = (positions[None, :] <= positions[:, None]) & (positions[None, :] < seq_len)
    scores = jnp.where(allowed[None], scores, NEG_BIG)
    attn_probs = jax.nn.softmax(scores, axis=-1).astype(jnp.bfloat16)
    attn_out = jnp.einsum("hqk,kc->qhc", attn_probs.astype(jnp.float32), v_act.astype(jnp.float32)).astype(jnp.bfloat16)
    mlp_out = (jax.nn.silu(gate_act.astype(jnp.float32)) * up_act.astype(jnp.float32)).astype(jnp.bfloat16)
    joined = jnp.concatenate([attn_out, mlp_out], axis=-1).reshape(SEQ_LEN, MODEL_SHARDS, SHARD_ROWS)
    w_groups = w_out_l.reshape(MODEL_SHARDS, SHARD_ROWS, D_MODEL)

    def add_group(running, group_pair):
        rows_in, w_rows = group_pair
        group_sum = jnp.dot(rows_in, w_rows, preferred_element_type=jnp.float32).astype(jnp.bfloat16)
        return running + group_sum.astype(jnp.float32), None

    z_sum, _ = lax.scan(add_group, jnp.zeros((SEQ_LEN, D_MODEL), jnp.float32), (jnp.swapaxes(joined, 0, 1), w_groups))
    return (x_f32 + z_sum).astype(jnp.bfloat16)


def reference(x, lengths, norm_gain, w_in, w_kv, w_out):
    seqs_x = x.reshape(N_MICRO * N_SEQS, SEQ_LEN, D_MODEL)
    seqs_len = lengths.reshape(N_MICRO * N_SEQS)

    def run_seq(seq_item):
        x_seq, seq_len = seq_item

        def one_layer(carry_x, weights):
            gain_l, w_in_l, w_kv_l, w_out_l = weights
            return layer_one_seq(carry_x, seq_len, gain_l, w_in_l, w_kv_l, w_out_l), None

        final_x, _ = lax.scan(one_layer, x_seq, (norm_gain, w_in, w_kv, w_out))
        return final_x

    y_all = lax.map(run_seq, (seqs_x, seqs_len))
    return y_all.reshape(N_MICRO, N_SEQS, SEQ_LEN, D_MODEL)
```

```python
import functools
import math

import jax
import jax.numpy as jnp
from jax import lax
from jax.experimental import pallas as pl
from jax.experimental.pallas import tpu as pltpu
from jax.sharding import PartitionSpec as P

MESH = pl.DeviceIdType.MESH
NORM_EPS = 1e-6
MASKED = -3e38
SIDE = 4
ROTATIONS = (("x", "y", "z"), ("y", "z", "x"), ("z", "x", "y"))
TILE = 256
DO_COMM = True
DO_COMPUTE = True


def mesh_kernel(dims, x_hbm, lens_ref, small_hbm, big_hbm, y_hbm,
                wsmall, wbig, xbuf, hbuf, kbuf, vbuf, acc, joined, zsend, zrecv, gain_buf,
                own_sem, wsend, wrecv, io_sem, hsend, hrecv, zs_sem, zr_sem):
    n_micro, n_layers, n_chunks, t_loc, d_model, head_dim, ff_head = dims
    n_total = n_layers * n_chunks
    pair_q, pair_f = 2 * head_dim, 2 * ff_head
    in_cols = pair_q + 2 * pair_f
    seq = 2 * t_loc
    me = lax.axis_index("data")
    core = lax.axis_index("model")
    pos = {"x": lax.rem(me, SIDE), "y": lax.rem(me // SIDE, SIDE), "z": me // (SIDE * SIDE)}
    stride = {"x": 1, "y": SIDE, "z": SIDE * SIDE}

    def shifted(axis, step):
        moved = lax.rem(pos[axis] + SIDE + step, SIDE)
        return moved, me + (moved - pos[axis]) * stride[axis]

    near = {(a, s): shifted(a, s) for a in "xyz" for s in (1, -1)}
    sibling = {"model": 1 - core}

    barrier = pltpu.get_barrier_semaphore()
    for key in near:
        pl.semaphore_signal(barrier, inc=1, device_id={"data": near[key][1]}, device_id_type=MESH)
    pl.semaphore_signal(barrier, inc=1, device_id=sibling, device_id_type=MESH)
    pl.semaphore_wait(barrier, 7)

    big_parts = ((0, pair_q + pair_f), (pair_q + pair_f, in_cols), (in_cols, wbig.shape[-1]))
    small_parts = ((0, 256), (256, 384), (384, 512))

    class Chunk:
        def __init__(self, buf, src, parts, sem_idx):
            self.buf, self.src, self.parts, self.sem = buf, src, parts, sem_idx

        def region(self, where, cols):
            return self.buf.at[where["z"], where["y"], where["x"], :, pl.ds(cols[0], cols[1] - cols[0])]

        def own(self):
            return pltpu.make_async_copy(self.src, self.buf.at[pos["z"], pos["y"], pos["x"]], own_sem.at[self.sem])

        def send(self, k):
            phase, second = k // 2, k % 2
            for rot, (lo, hi) in zip(ROTATIONS, self.parts):
                axis = rot[phase]
                mid = lo + (((hi - lo) // 128 + 1) // 2) * 128
                for sign in (1, -1):
                    where = {a: slice(None) for a in rot[:phase]}
                    where.update({a: pos[a] for a in rot[phase:]})
                    cols = (lo, hi)
                    if second:
                        where[axis] = near[axis, -sign][0]
                        if phase == 0:
                            cols = (lo, mid) if sign == 1 else (mid, hi)
                            if cols[0] == cols[1]:
                                continue
                        else:
                            where[rot[0]] = pl.ds(0, 2) if sign == 1 else pl.ds(2, 2)
                    dst = self.region(where, cols)
                    src = self.src.at[:, pl.ds(cols[0], cols[1] - cols[0])] if k == 0 else dst
                    pltpu.make_async_remote_copy(
                        src_ref=src, dst_ref=dst, send_sem=wsend.at[self.sem, k], recv_sem=wrecv.at[self.sem, k],
                        device_id={"data": near[axis, sign][1]}, device_id_type=MESH).start()

        def bytes_of(self, k):
            ref = (self.buf.at[0, 0, pl.ds(0, 2)], self.buf.at[0, 0, 0], self.buf.at[0, pl.ds(0, 2)],
                   self.buf.at[0, 0], self.buf.at[pl.ds(0, 2)], self.buf.at[0])[k]
            return pltpu.make_async_remote_copy(
                src_ref=ref, dst_ref=ref, send_sem=wsend.at[self.sem, k], recv_sem=wrecv.at[self.sem, k],
                device_id={"data": near["x", 1][1]}, device_id_type=MESH)

        def step(self, k):
            if not DO_COMM:
                return
            if k == 0:
                self.own().start()
            else:
                self.bytes_of(k - 1).wait_recv()
            if k == 2:
                self.own().wait()
            if k < 6:
                self.send(k)

        def finish(self):
            if not DO_COMM:
                return
            for k in range(6):
                self.bytes_of(k).wait_send()

    small = Chunk(wsmall, small_hbm, small_parts, n_total)

    def big(n):
        return Chunk(wbig.at[n], big_hbm.at[n], big_parts, n)

    def step(n, k):
        if isinstance(n, int):
            if n < n_total:
                big(n).step(k)
        else:
            @pl.when(n < n_total)
            def _():
                big(n).step(k)

    def load_x(m):
        return pltpu.make_async_copy(x_hbm.at[m], xbuf.at[m], io_sem.at[m])

    def store_y(m):
        return pltpu.make_async_copy(xbuf.at[m], y_hbm.at[m], io_sem.at[m])

    def send_h(m):
        rows = hbuf.at[m, pl.ds(pl.multiple_of(core * t_loc, t_loc), t_loc)]
        return pltpu.make_async_remote_copy(src_ref=rows, dst_ref=rows, send_sem=hsend.at[m], recv_sem=hrecv.at[m],
                                            device_id=sibling, device_id_type=MESH)

    def send_z(m):
        return pltpu.make_async_remote_copy(src_ref=zsend.at[m], dst_ref=zrecv.at[m], send_sem=zs_sem.at[m],
                                            recv_sem=zr_sem.at[m], device_id=sibling, device_id_type=MESH)

    norm_rows = 32

    def norm(m, layer):
        gain = gain_buf[layer]

        def rows_of(r, carry):
            at = pl.multiple_of(r * norm_rows, norm_rows)
            x_f32 = xbuf[m, pl.ds(at, norm_rows), :].astype(jnp.float32)
            centered = x_f32 - jnp.mean(x_f32, axis=-1, keepdims=True)
            variance = jnp.mean(centered * centered, axis=-1, keepdims=True)
            h_act = (centered * lax.rsqrt(variance + NORM_EPS) * gain).astype(jnp.bfloat16)
            hbuf[m, pl.ds(pl.multiple_of(core * t_loc + at, norm_rows), norm_rows), :] = h_act
            return carry

        lax.fori_loop(0, t_loc // norm_rows, rows_of, 0)

    def keys_values(m, layer):
        w_kv = wsmall[:, :, :, :, pl.ds(pl.multiple_of(layer * 256, 128), 128)].reshape(d_model, 2 * head_dim)
        lane = lax.broadcasted_iota(jnp.int32, (TILE, 2 * head_dim), 1)
        low = lane < head_dim
        length = lens_ref[m]

        def rows_of(r, carry):
            at = pl.multiple_of(r * TILE, TILE)
            kv_f32 = jnp.dot(hbuf[m, pl.ds(at, TILE), :], w_kv, preferred_element_type=jnp.float32)
            kv_f32 = kv_f32.astype(jnp.bfloat16).astype(jnp.float32)
            vk_f32 = pltpu.roll(kv_f32, head_dim, 1)
            key_pos = at + lax.broadcasted_iota(jnp.int32, (TILE, 2 * head_dim), 0)
            bias = jnp.where(key_pos < length, 0.0, MASKED)
            k_low = jnp.where(low, kv_f32, jnp.where(lane == head_dim, bias, 0.0))
            k_high = jnp.where(low, jnp.where(lane == 0, bias, 0.0), vk_f32)
            kbuf[m, 0, pl.ds(at, TILE), :] = k_low.astype(jnp.bfloat16)
            kbuf[m, 1, pl.ds(at, TILE), :] = k_high.astype(jnp.bfloat16)
            vbuf[m, 0, pl.ds(at, TILE), :] = jnp.where(low, vk_f32, 0.0).astype(jnp.bfloat16)
            vbuf[m, 1, pl.ds(at, TILE), :] = jnp.where(low, 0.0, kv_f32).astype(jnp.bfloat16)
            return carry

        lax.fori_loop(0, seq // TILE, rows_of, 0)

    exp_scale = (1.0 / math.sqrt(head_dim)) * math.log2(math.e)

    def body(n, c, m):
        lane = lax.broadcasted_iota(jnp.int32, (TILE, pair_q), 1)
        tri = (lax.broadcasted_iota(jnp.int32, (TILE, TILE), 1) <= lax.broadcasted_iota(jnp.int32, (TILE, TILE), 0))
        for i in range(seq // TILE):
            rows = pl.ds(i * TILE, TILE)
            n_keys = (i + 1) * TILE
            h_rows = hbuf[m, rows, :]

            def weight(lo, hi):
                return wbig[n, :, :, :, :, lo:hi].reshape(d_model, hi - lo)

            q = jnp.dot(h_rows, weight(0, pair_q), preferred_element_type=jnp.float32).astype(jnp.bfloat16)
            one = jnp.ones((), jnp.bfloat16)
            zero = jnp.zeros((), jnp.bfloat16)
            q_low = jnp.where(lane < head_dim, q, jnp.where(lane == head_dim, one, zero))
            q_high = jnp.where(lane < head_dim, jnp.where(lane == 0, one, zero), q)
            scores = [lax.dot_general(q_aug, kbuf[m, side, 0:n_keys, :], (((1,), (1,)), ((), ())),
                                      preferred_element_type=jnp.float32)
                      for side, q_aug in ((0, q_low), (1, q_high))]
            gate = jnp.dot(h_rows, weight(pair_q, pair_q + pair_f), preferred_element_type=jnp.float32)
            up = jnp.dot(h_rows, weight(pair_q + pair_f, in_cols), preferred_element_type=jnp.float32)
            out = None
            for side in (0, 1):
                s = scores[side]
                diag = jnp.where(tri, s[:, n_keys - TILE:], MASKED)
                s = diag if i == 0 else jnp.concatenate([s[:, :n_keys - TILE], diag], axis=1)
                top = jnp.max(s, axis=1, keepdims=True)
                e = jnp.exp2((s - top) * exp_scale)
                p = (e * (1.0 / jnp.sum(e, axis=1, keepdims=True))).astype(jnp.bfloat16)
                o = jnp.dot(p, vbuf[m, side, 0:n_keys, :], preferred_element_type=jnp.float32)
                out = o if out is None else out + o
            joined[rows, 0:pair_q] = out.astype(jnp.bfloat16)
            gate = gate.astype(jnp.bfloat16).astype(jnp.float32)
            up = up.astype(jnp.bfloat16).astype(jnp.float32)
            half = 0.5 * gate
            joined[rows, pair_q:] = ((half + half * jnp.tanh(half)) * up).astype(jnp.bfloat16)
            w_out = wbig[n, :, :, :, :, in_cols:].reshape(d_model, pair_q + pair_f)
            acc[m, rows, :] += lax.dot_general(joined[rows, :], w_out, (((1,), (1,)), ((), ())),
                                               preferred_element_type=jnp.float32)

    def stage_z(m):
        def rows_of(r, carry):
            at = pl.multiple_of(r * 64, 64)
            other = pl.multiple_of((1 - core) * t_loc + at, 64)
            zsend[m, pl.ds(at, 64), :] = acc[m, pl.ds(other, 64), :].astype(jnp.bfloat16)
            return carry

        lax.fori_loop(0, t_loc // 64, rows_of, 0)
        send_z(m).start()

    def add_z(m):
        send_z(m).wait_recv()

        def rows_of(r, carry):
            at = pl.multiple_of(r * 64, 64)
            mine = pl.multiple_of(core * t_loc + at, 64)
            z_own = acc[m, pl.ds(mine, 64), :].astype(jnp.bfloat16).astype(jnp.float32)
            z_sum = z_own + zrecv[m, pl.ds(at, 64), :].astype(jnp.float32)
            xbuf[m, pl.ds(at, 64), :] = (xbuf[m, pl.ds(at, 64), :].astype(jnp.float32) + z_sum).astype(jnp.bfloat16)
            return carry

        lax.fori_loop(0, t_loc // 64, rows_of, 0)
        send_z(m).wait_send()

    for m in range(n_micro):
        load_x(m).start()
    small.step(0), step(0, 0), step(1, 0)
    small.step(1), step(0, 1), step(1, 1)
    small.step(2), step(0, 2)
    small.step(3), step(0, 3)
    small.step(4), step(0, 4)
    small.step(5), step(1, 2), step(2, 0)
    small.step(6), step(1, 3), step(2, 1)
    step(0, 5)

    for m in range(n_micro):
        load_x(m).wait()
    if DO_COMPUTE:
        for layer in range(n_layers):
            spread = wsmall[:, :, :, :, layer * 256 + 128:layer * 256 + 256].astype(jnp.float32).reshape(8, 128, 128)
            for k in range(8):
                gain_buf[layer, :, k * 128:(k + 1) * 128] = jnp.sum(spread[k], axis=0, keepdims=True)

    def layer_loop(layer, carry):
        if DO_COMPUTE:
            for m in range(n_micro):
                @pl.when(layer > 0)
                def _():
                    add_z(m)

                norm(m, layer)
                send_h(m).start()
            for m in range(n_micro):
                def clear(r, carry):
                    acc[m, pl.ds(pl.multiple_of(r * 64, 64), 64), :] = jnp.zeros((64, d_model), jnp.float32)
                    return carry

                lax.fori_loop(0, seq // 64, clear, 0)
                send_h(m).wait_recv()
                keys_values(m, layer)
            for m in range(n_micro):
                send_h(m).wait_send()

        def chunk_loop(it, carry):
            c, m = it // n_micro, lax.rem(it, n_micro)
            n = layer * n_chunks + c

            @pl.when(m == 0)
            def _():
                step(n, 6)
                step(n + 1, 4)
                step(n + 2, 2)
                step(n + 3, 0)

            @pl.when(m == 1)
            def _():
                step(n + 1, 5)
                step(n + 2, 3)
                step(n + 3, 1)

            if DO_COMPUTE:
                body(n, c, m)

                @pl.when(c == n_chunks - 1)
                def _():
                    stage_z(m)
            return carry

        lax.fori_loop(0, n_chunks * n_micro, chunk_loop, 0)
        return carry

    lax.fori_loop(0, n_layers, layer_loop, 0)
    for m in range(n_micro):
        if DO_COMPUTE:
            add_z(m)
        store_y(m).start()
    small.finish()

    def finish(n, carry):
        big(n).finish()
        return carry

    lax.fori_loop(0, n_total, finish, 0)
    for m in range(n_micro):
        store_y(m).wait()


def run_kernel(x_loc, lens, small, big, dims):
    n_micro, n_layers, n_chunks, t_loc, d_model, head_dim, ff_head = dims
    n_total = n_layers * n_chunks
    seq = 2 * t_loc
    any_spec = pl.BlockSpec(memory_space=pl.ANY)
    bf16 = jnp.bfloat16
    return pl.pallas_call(
        functools.partial(mesh_kernel, dims),
        out_shape=jax.ShapeDtypeStruct((n_micro, t_loc, d_model), bf16),
        in_specs=[any_spec, pl.BlockSpec(memory_space=pltpu.SMEM), any_spec, any_spec],
        out_specs=any_spec,
        scratch_shapes=[
            pltpu.VMEM((SIDE, SIDE, SIDE) + small.shape, bf16),
            pltpu.VMEM((n_total, SIDE, SIDE, SIDE) + big.shape[1:], bf16),
            pltpu.VMEM((n_micro, t_loc, d_model), bf16),
            pltpu.VMEM((n_micro, seq, d_model), bf16),
            pltpu.VMEM((n_micro, 2, seq, 2 * head_dim), bf16),
            pltpu.VMEM((n_micro, 2, seq, 2 * head_dim), bf16),
            pltpu.VMEM((n_micro, seq, d_model), jnp.float32),
            pltpu.VMEM((seq, 2 * (head_dim + ff_head)), bf16),
            pltpu.VMEM((n_micro, t_loc, d_model), bf16),
            pltpu.VMEM((n_micro, t_loc, d_model), bf16),
            pltpu.VMEM((n_layers, 1, d_model), jnp.float32),
            pltpu.SemaphoreType.DMA((n_total + 1,)),
            pltpu.SemaphoreType.DMA((n_total + 1, 6)),
            pltpu.SemaphoreType.DMA((n_total + 1, 6)),
            pltpu.SemaphoreType.DMA((n_micro,)),
            pltpu.SemaphoreType.DMA((n_micro,)),
            pltpu.SemaphoreType.DMA((n_micro,)),
            pltpu.SemaphoreType.DMA((n_micro,)),
            pltpu.SemaphoreType.DMA((n_micro,)),
        ],
        compiler_params=pltpu.CompilerParams(collective_id=0, has_side_effects=True, vmem_limit_bytes=67043328),
    )(x_loc, lens, small, big)


def pack(gain, w_in, w_kv, w_out, n_chunks):
    n_layers, rows, in_cols = w_in.shape
    head_dim = w_kv.shape[2] // 2
    out_rows = w_out.shape[1]
    heads = (out_rows * 2 - in_cols) // head_dim
    ff_head = out_rows // heads - head_dim
    w_in5 = w_in.reshape(n_layers, rows, n_chunks, 2, head_dim + 2 * ff_head)
    w_out5 = jnp.swapaxes(w_out, 1, 2).reshape(n_layers, rows, n_chunks, 2, head_dim + ff_head)
    lead = (n_layers, rows, n_chunks)
    big = jnp.concatenate([
        w_in5[..., :head_dim].reshape(lead + (-1,)),
        w_in5[..., head_dim:head_dim + ff_head].reshape(lead + (-1,)),
        w_in5[..., head_dim + ff_head:].reshape(lead + (-1,)),
        w_out5[..., :head_dim].reshape(lead + (-1,)),
        w_out5[..., head_dim:].reshape(lead + (-1,)),
    ], axis=-1)
    big = jnp.transpose(big, (0, 2, 1, 3)).reshape(n_layers * n_chunks, rows, -1)
    lane = rows * lax.rem(lax.axis_index("data"), 128 // rows)
    here = (lane + lax.broadcasted_iota(jnp.int32, (rows, 128), 0)) == lax.broadcasted_iota(jnp.int32, (rows, 128), 1)
    pieces = []
    for layer in range(n_layers):
        pieces.append(w_kv[layer])
        pieces.append(jnp.where(here, gain[layer][:, None], jnp.zeros((), gain.dtype)))
    return jnp.concatenate(pieces, axis=1), big, head_dim, ff_head


def solution(mesh):
    act_spec = P(None, ("part", "data"), "model", None)
    n_chunks = 4

    def local_fn(x_blk, len_blk, gain_blk, w_in_blk, w_kv_blk, w_out_blk):
        n_micro, _, t_loc, d_model = x_blk.shape
        small, big, head_dim, ff_head = pack(gain_blk, w_in_blk, w_kv_blk, w_out_blk, n_chunks)
        dims = (n_micro, gain_blk.shape[0], n_chunks, t_loc, d_model, head_dim, ff_head)
        y = run_kernel(x_blk.reshape(n_micro, t_loc, d_model), len_blk.reshape(n_micro), small, big, dims)
        return y.reshape(x_blk.shape)

    return jax.shard_map(
        local_fn,
        mesh=mesh,
        in_specs=(act_spec, P(None, ("part", "data")), P(None, "data"), P(None, "data", "model"), P(None, "data", None), P(None, "model", "data")),
        out_specs=act_spec,
        check_vma=False,
    )
```

```python
import functools
import math

import jax
import jax.numpy as jnp
from jax import lax
from jax.experimental import pallas as pl
from jax.experimental.pallas import tpu as pltpu
from jax.sharding import PartitionSpec as P

MESH = pl.DeviceIdType.MESH
NORM_EPS = 1e-6
MASKED = -3e38
SIDE = 4
ROTATIONS = (("x", "y", "z"), ("y", "z", "x"), ("z", "x", "y"))
TILE = 256
BLOCK = 128
N_COMM = 99
DO_COMM = True
DO_COMPUTE = True


def mesh_kernel(dims, x_hbm, lens_ref, gain_ref, kv_ref, w_in_hbm, w_out_hbm, y_hbm,
                small, wsmall, wbig, xbuf, hbuf, kbuf, vbuf, acc, joined, zsend, zrecv, gain_buf,
                own_sem, wsend, wrecv, io_sem, hsend, hrecv, zs_sem, zr_sem):
    n_micro, n_layers, n_chunks, t_loc, d_model, head_dim, ff_head = dims
    n_total = n_layers * n_chunks
    pair_q, pair_f = 2 * head_dim, 2 * ff_head
    in_cols = pair_q + 2 * pair_f
    seq = 2 * t_loc
    me = lax.axis_index("data")
    core = lax.axis_index("model")
    pos = {"x": lax.rem(me, SIDE), "y": lax.rem(me // SIDE, SIDE), "z": me // (SIDE * SIDE)}
    stride = {"x": 1, "y": SIDE, "z": SIDE * SIDE}

    def shifted(axis, step):
        moved = lax.rem(pos[axis] + SIDE + step, SIDE)
        return moved, me + (moved - pos[axis]) * stride[axis]

    near = {(a, s): shifted(a, s) for a in "xyz" for s in (1, -1)}
    far = {a: shifted(a, 2) for a in "xyz"}
    sibling = {"model": 1 - core}

    barrier = pltpu.get_barrier_semaphore()
    for key in near:
        pl.semaphore_signal(barrier, inc=1, device_id={"data": near[key][1]}, device_id_type=MESH)
    for axis in "xyz":
        pl.semaphore_signal(barrier, inc=1, device_id={"data": far[axis][1]}, device_id_type=MESH)
    pl.semaphore_signal(barrier, inc=1, device_id=sibling, device_id_type=MESH)

    def load_x(m):
        return pltpu.make_async_copy(x_hbm.at[m], xbuf.at[m], io_sem.at[m])

    for m in range(n_micro):
        load_x(m).start()

    n_rows = kv_ref.shape[1]
    for layer in range(n_layers):
        small[:, layer * 128:(layer + 1) * 128] = kv_ref[layer]
    spread = (lax.rem(lax.broadcasted_iota(jnp.int32, (n_rows, 128), 1), n_rows)
              == lax.broadcasted_iota(jnp.int32, (n_rows, 128), 0)).astype(jnp.float32).astype(jnp.bfloat16)
    gains = jnp.dot(gain_ref[...], spread, preferred_element_type=jnp.float32)
    feature = lax.broadcasted_iota(jnp.int32, (n_rows, 128), 1) - n_rows * lax.rem(me, 128 // n_rows)
    row = lax.broadcasted_iota(jnp.int32, (n_rows, 128), 0)
    block = jnp.zeros((n_rows, 128), jnp.float32)
    for layer in range(n_layers):
        block = jnp.where(lax.rem(feature + layer, n_rows) == row, jnp.where(feature >= 0, jnp.where(
            feature < n_rows, gains[layer:layer + 1, :], block), block), block)
    small[:, n_layers * 128:] = block.astype(jnp.bfloat16)
    pl.semaphore_wait(barrier, 10)

    cut = 128 * ((in_cols // 128 + 1) // 2)
    out_cols = pair_q + pair_f
    big_parts = ((0, cut), (cut, in_cols), (in_cols, in_cols + out_cols))
    small_parts = ((0, 128), (128, 256), (256, 384))

    class Chunk:
        def __init__(self, buf, sources, parts, sem_idx, direct=()):
            self.buf, self.sources, self.parts, self.sem, self.direct = buf, sources, parts, sem_idx, direct

        def region(self, where, cols):
            return self.buf.at[where["z"], where["y"], where["x"], :, pl.ds(cols[0], cols[1] - cols[0])]

        def own(self):
            copies = []
            if self is first:
                return copies
            for j, (src, lo, hi) in enumerate(self.sources):
                dst = self.buf.at[pos["z"], pos["y"], pos["x"], :, pl.ds(lo, hi - lo)]
                copies.append(pltpu.make_async_copy(src, dst, own_sem.at[self.sem, j]))
            return copies

        def source(self, cols):
            for src, lo, hi in self.sources:
                if lo <= cols[0] and cols[1] <= hi:
                    return src.at[:, pl.ds(cols[0] - lo, cols[1] - cols[0])]

        def send(self, k):
            phase, second = k // 2, k % 2
            direct = phase in self.direct
            if direct and second:
                return
            for rot, (lo, hi) in zip(ROTATIONS, self.parts):
                axis = rot[phase]
                mid = lo + (((hi - lo) // 128 + 1) // 2) * 128
                for sign in (1, -1, 2)[:3 if direct else 2]:
                    where = {a: slice(None) for a in rot[:phase]}
                    where.update({a: pos[a] for a in rot[phase:]})
                    cols = (lo, hi)
                    if second:
                        where[axis] = near[axis, -sign][0]
                        if phase == 0:
                            cols = (lo, mid) if sign == 1 else (mid, hi)
                            if cols[0] == cols[1]:
                                continue
                        else:
                            where[rot[0]] = pl.ds(0, 2) if sign == 1 else pl.ds(2, 2)
                    dst = self.region(where, cols)
                    src = self.source(cols) if k == 0 else dst
                    pltpu.make_async_remote_copy(
                        src_ref=src, dst_ref=dst, send_sem=wsend.at[self.sem, k], recv_sem=wrecv.at[self.sem, k],
                        device_id={"data": far[axis][1] if sign == 2 else near[axis, sign][1]}, device_id_type=MESH).start()

        def bytes_of(self, k):
            count = 1 if k % 2 else 3 if k // 2 in self.direct else 2
            ref = (self.buf.at[0, 0, pl.ds(0, count)], self.buf.at[0, pl.ds(0, count)], self.buf.at[pl.ds(0, count)])[k // 2]
            return pltpu.make_async_remote_copy(
                src_ref=ref, dst_ref=ref, send_sem=wsend.at[self.sem, k], recv_sem=wrecv.at[self.sem, k],
                device_id={"data": near["x", 1][1]}, device_id_type=MESH)

        def step(self, k):
            if not DO_COMM:
                return
            if k == 0:
                for copy in self.own():
                    copy.start()
            elif k % 2 or k // 2 - 1 not in self.direct:
                self.bytes_of(k - 1).wait_recv()
            else:
                self.bytes_of(k - 2).wait_recv()
            if k == 2:
                for copy in self.own():
                    copy.wait()
            if k < 6:
                self.send(k)

        def finish(self):
            if not DO_COMM:
                return
            for k in range(6):
                if k % 2 == 0 or k // 2 not in self.direct:
                    self.bytes_of(k).wait_send()

    first = Chunk(wsmall, ((small, 0, 384),), small_parts, n_total, direct=(0, 1))

    def big(n):
        layer, c = n // n_chunks, n % n_chunks if isinstance(n, int) else lax.rem(n, n_chunks)

        def piece(ref, width):
            at = c * width if isinstance(c, int) else pl.multiple_of(c * width, 128)
            return ref.at[layer, :, pl.ds(at, width)]

        return Chunk(wbig.at[n], ((piece(w_in_hbm, in_cols), 0, in_cols),
                                  (piece(w_out_hbm, out_cols), in_cols, in_cols + out_cols)), big_parts, n,
                     direct=(0,) if isinstance(n, int) and n == 0 else ())

    def step(n, k):
        if isinstance(n, int):
            if n < min(n_total, N_COMM):
                big(n).step(k)
        else:
            @pl.when(n < min(n_total, N_COMM))
            def _():
                big(n).step(k)

    def store_y(m):
        return pltpu.make_async_copy(xbuf.at[m], y_hbm.at[m], io_sem.at[m])

    n_blocks = t_loc // BLOCK

    def send_h(m, r):
        rows = hbuf.at[m, pl.ds(pl.multiple_of(core * t_loc + r * BLOCK, BLOCK), BLOCK)]
        return pltpu.make_async_remote_copy(src_ref=rows, dst_ref=rows, send_sem=hsend.at[m, r], recv_sem=hrecv.at[m, r],
                                            device_id=sibling, device_id_type=MESH)

    def send_z(m, r):
        rows = pl.ds(pl.multiple_of(r * BLOCK, BLOCK), BLOCK)
        return pltpu.make_async_remote_copy(src_ref=zsend.at[m, rows], dst_ref=zrecv.at[m, rows], send_sem=zs_sem.at[m, r],
                                            recv_sem=zr_sem.at[m, r], device_id=sibling, device_id_type=MESH)

    def add_z(m, r):
        rows = pl.ds(pl.multiple_of(r * BLOCK, BLOCK), BLOCK)
        mine = pl.ds(pl.multiple_of(core * t_loc + r * BLOCK, BLOCK), BLOCK)
        send_z(m, r).wait_recv()
        z_own = acc[m, mine, :].astype(jnp.bfloat16).astype(jnp.float32)
        y = (xbuf[m, rows, :].astype(jnp.float32) + (z_own + zrecv[m, rows, :].astype(jnp.float32))).astype(jnp.bfloat16)
        xbuf[m, rows, :] = y
        acc[m, mine, :] = jnp.zeros((BLOCK, d_model), jnp.float32)
        send_z(m, r).wait_send()

    def norm(m, layer, after_z):
        def block_of(r, carry):
            if after_z:
                add_z(m, r)
            x_f32 = xbuf[m, pl.ds(pl.multiple_of(r * BLOCK, BLOCK), BLOCK), :].astype(jnp.float32)
            centered = x_f32 - jnp.mean(x_f32, axis=-1, keepdims=True)
            variance = jnp.mean(centered * centered, axis=-1, keepdims=True)
            h_act = (centered * lax.rsqrt(variance + NORM_EPS) * gain_buf[layer]).astype(jnp.bfloat16)
            hbuf[m, pl.ds(pl.multiple_of(core * t_loc + r * BLOCK, BLOCK), BLOCK), :] = h_act

            @pl.when(r > 0)
            def _():
                send_h(m, r - 1).start()
            return carry

        lax.fori_loop(0, n_blocks, block_of, 0)
        send_h(m, n_blocks - 1).start()

    def keys_values(m, layer):
        w_kv = wsmall[:, :, :, :, pl.ds(pl.multiple_of(layer * 128, 128), 128)].reshape(d_model, 2 * head_dim)
        lane = lax.broadcasted_iota(jnp.int32, (TILE, 2 * head_dim), 1)
        low = lane < head_dim
        length = lens_ref[m]

        def half(base):
            for t in range(t_loc // TILE):
                at = pl.multiple_of(base + t * TILE, TILE)
                rows = pl.ds(at, TILE)
                kv_f32 = jnp.dot(hbuf[m, rows, :], w_kv, preferred_element_type=jnp.float32)
                kv_f32 = kv_f32.astype(jnp.bfloat16).astype(jnp.float32)
                vk_f32 = pltpu.roll(kv_f32, head_dim, 1)
                key_pos = at + lax.broadcasted_iota(jnp.int32, (TILE, 2 * head_dim), 0)
                bias = jnp.where(key_pos < length, 0.0, MASKED)
                k_low = jnp.where(low, kv_f32, jnp.where(lane == head_dim, bias, 0.0))
                k_high = jnp.where(low, jnp.where(lane == 0, bias, 0.0), vk_f32)
                kbuf[m, 0, rows, :] = k_low.astype(jnp.bfloat16)
                kbuf[m, 1, rows, :] = k_high.astype(jnp.bfloat16)
                vbuf[m, 0, rows, :] = jnp.where(low, vk_f32, 0.0).astype(jnp.bfloat16)
                vbuf[m, 1, rows, :] = jnp.where(low, 0.0, kv_f32).astype(jnp.bfloat16)

        half(core * t_loc)
        for r in range(n_blocks):
            send_h(m, r).wait_recv()
        half((1 - core) * t_loc)
        for r in range(n_blocks):
            send_h(m, r).wait_send()

    exp_scale = (1.0 / math.sqrt(head_dim)) * math.log2(math.e)

    def body(n, m):
        lane = lax.broadcasted_iota(jnp.int32, (TILE, 2 * head_dim), 1)
        low = lane < head_dim
        seen = (lax.broadcasted_iota(jnp.int32, (TILE, TILE), 0) >= lax.broadcasted_iota(jnp.int32, (TILE, TILE), 1))
        w_in = wbig[n, :, :, :, :, :in_cols].reshape(d_model, in_cols)
        w_out = wbig[n, :, :, :, :, in_cols:].reshape(d_model, out_cols)
        one = jnp.ones((), jnp.bfloat16)
        zero = jnp.zeros((), jnp.bfloat16)
        unit = head_dim + 2 * ff_head
        n_tiles = seq // TILE
        proj, scores = {}, {}

        def rows(i):
            return slice(i * TILE, (i + 1) * TILE)

        def project(i):
            proj[i] = jnp.dot(hbuf[m, rows(i), :], w_in, preferred_element_type=jnp.float32).astype(jnp.bfloat16)

        def score(i):
            n_keys = (i + 1) * TILE
            at = unit - head_dim
            q_aug = (jnp.where(low, proj[i][:, :2 * head_dim], jnp.where(lane == head_dim, one, zero)),
                     jnp.where(low, jnp.where(lane == 0, one, zero), proj[i][:, at:at + 2 * head_dim]))
            for side in (0, 1):
                s = lax.dot_general(q_aug[side], kbuf[m, side, 0:n_keys, :], (((1,), (1,)), ((), ())),
                                    preferred_element_type=jnp.float32)
                diag = jnp.where(seen, s[:, n_keys - TILE:], MASKED)
                scores[i, side] = diag if i == 0 else jnp.concatenate([s[:, :n_keys - TILE], diag], axis=1)

        def softmax(s):
            top = jnp.max(s, axis=1, keepdims=True)
            e = jnp.exp2((s - top) * exp_scale)
            return (e * (1.0 / jnp.sum(e, axis=1, keepdims=True))).astype(jnp.bfloat16)

        def mlp(i, g_at, u_at, width):
            gate = proj[i][:, g_at:g_at + width].astype(jnp.float32)
            up = proj[i][:, u_at:u_at + width].astype(jnp.float32)
            half = 0.5 * gate
            return ((half + half * jnp.tanh(half)) * up).astype(jnp.bfloat16)

        def join(i):
            n_keys = (i + 1) * TILE
            probs = [softmax(scores.pop((i, side))) for side in (0, 1)]
            first = mlp(i, 0, ff_head, ff_head + 2 * head_dim)
            joined[rows(i), 2 * head_dim:ff_head] = first[:, 2 * head_dim:ff_head]
            joined[rows(i), ff_head + 2 * head_dim:] = mlp(i, unit + head_dim, unit + head_dim + ff_head, ff_head)
            outs = [jnp.dot(probs[side], vbuf[m, side, 0:n_keys, :], preferred_element_type=jnp.float32) for side in (0, 1)]
            pair = (outs[0] + outs[1]).astype(jnp.bfloat16)
            joined[rows(i), 0:2 * head_dim] = jnp.where(low, pair, first[:, :2 * head_dim])
            joined[rows(i), ff_head:ff_head + 2 * head_dim] = jnp.where(low, first[:, ff_head:], pair)

        def project_out(i):
            acc[m, rows(i), :] += lax.dot_general(joined[rows(i), :], w_out, (((1,), (1,)), ((), ())),
                                                  preferred_element_type=jnp.float32)

        order = list(range(n_tiles))[::-1]
        project(order[0])
        score(order[0])
        for at, i in enumerate(order):
            following = order[at + 1:at + 2]
            for j in following:
                project(j)
            join(i)
            for j in following:
                score(j)
            project_out(i)

    def stage_z(m):
        def block_of(r, carry):
            other = pl.ds(pl.multiple_of((1 - core) * t_loc + r * BLOCK, BLOCK), BLOCK)
            zsend[m, pl.ds(pl.multiple_of(r * BLOCK, BLOCK), BLOCK), :] = acc[m, other, :].astype(jnp.bfloat16)
            acc[m, other, :] = jnp.zeros((BLOCK, d_model), jnp.float32)

            @pl.when(r > 0)
            def _():
                send_z(m, r - 1).start()
            return carry

        lax.fori_loop(0, n_blocks, block_of, 0)
        send_z(m, n_blocks - 1).start()

    def boundary(layer, after_z):
        for m in range(n_micro):
            norm(m, layer, after_z)
        for m in range(n_micro):
            keys_values(m, layer)

    if DO_COMM:
        wsmall[pos["z"], pos["y"], pos["x"]] = small[...]
    first.step(0), step(0, 0), step(1, 0), step(2, 0)
    first.step(2), step(0, 2), step(1, 1), step(2, 1)
    first.step(4), step(0, 3), step(1, 2), step(2, 2)
    first.step(5), step(0, 4), step(1, 3), step(2, 3), step(3, 0), step(4, 0)
    if DO_COMPUTE:
        def clear(r, carry):
            for m in range(n_micro):
                acc[m, pl.ds(pl.multiple_of(r * 64, 64), 64), :] = jnp.zeros((64, d_model), jnp.float32)
            return carry

        lax.fori_loop(0, seq // 64, clear, 0)
    first.step(6)
    for m in range(n_micro):
        load_x(m).wait()
    if DO_COMPUTE:
        table = wsmall[:, :, :, :, n_layers * 128:].astype(jnp.float32).reshape(d_model // 128, 128, 128)
        lane = lax.broadcasted_iota(jnp.int32, (128, 128), 1)
        row = lax.broadcasted_iota(jnp.int32, (128, 128), 0)
        for layer in range(n_layers):
            mine = lax.rem(lane + layer, n_rows) == lax.rem(row, n_rows)
            for k in range(d_model // 128):
                gain_buf[layer, :, k * 128:(k + 1) * 128] = jnp.sum(jnp.where(mine, table[k], 0.0), axis=0, keepdims=True)
        norm(0, 0, False)
        norm(1, 0, False)
    step(0, 5), step(3, 1), step(4, 1), step(1, 4), step(3, 2), step(5, 0)
    if DO_COMPUTE:
        keys_values(0, 0)
        keys_values(1, 0)

    def layer_loop(layer, carry):
        if DO_COMPUTE:
            @pl.when(layer > 0)
            def _():
                boundary(layer, True)

        def chunk_loop(it, carry):
            c, m = it // n_micro, lax.rem(it, n_micro)
            n = layer * n_chunks + c

            @pl.when(m == 0)
            def _():
                step(n, 6)

            @pl.when(m == 1)
            def _():
                step(n + 1, 5)
                step(n + 2, 4)
                step(n + 3, 3)
                step(n + 4, 2)
                step(n + 5, 1)
                step(n + 6, 0)

            if DO_COMPUTE:
                body(n, m)

                @pl.when(c == n_chunks - 1)
                def _():
                    stage_z(m)
            return carry

        lax.fori_loop(0, n_chunks * n_micro, chunk_loop, 0)
        return carry

    lax.fori_loop(0, n_layers, layer_loop, 0)
    for m in range(n_micro):
        if DO_COMPUTE:
            for r in range(n_blocks):
                add_z(m, r)
        store_y(m).start()
    first.finish()
    step_zero = big(0)
    if N_COMM > 0:
        step_zero.finish()

    def finish(n, carry):
        big(n).finish()
        return carry

    lax.fori_loop(1, min(n_total, N_COMM), finish, 0)
    for m in range(n_micro):
        store_y(m).wait()


def run_kernel(x_loc, lens, gain, w_kv, w_in, w_out, dims):
    n_micro, n_layers, n_chunks, t_loc, d_model, head_dim, ff_head = dims
    n_total = n_layers * n_chunks
    seq = 2 * t_loc
    any_spec = pl.BlockSpec(memory_space=pl.ANY)
    vmem_spec = pl.BlockSpec(memory_space=pltpu.VMEM)
    bf16 = jnp.bfloat16
    rows = w_in.shape[1]
    small_cols = (n_layers + 1) * 128
    n_blocks = t_loc // BLOCK
    return pl.pallas_call(
        functools.partial(mesh_kernel, dims),
        out_shape=jax.ShapeDtypeStruct((n_micro, t_loc, d_model), bf16),
        in_specs=[any_spec, pl.BlockSpec(memory_space=pltpu.SMEM), vmem_spec, vmem_spec, any_spec, any_spec],
        out_specs=any_spec,
        scratch_shapes=[
            pltpu.VMEM((rows, small_cols), bf16),
            pltpu.VMEM((SIDE, SIDE, SIDE, rows, small_cols), bf16),
            pltpu.VMEM((n_total, SIDE, SIDE, SIDE, w_in.shape[1], (w_in.shape[2] + w_out.shape[2]) // n_chunks), bf16),
            pltpu.VMEM((n_micro, t_loc, d_model), bf16),
            pltpu.VMEM((n_micro, seq, d_model), bf16),
            pltpu.VMEM((n_micro, 2, seq, 2 * head_dim), bf16),
            pltpu.VMEM((n_micro, 2, seq, 2 * head_dim), bf16),
            pltpu.VMEM((n_micro, seq, d_model), jnp.float32),
            pltpu.VMEM((seq, 2 * (head_dim + ff_head)), bf16),
            pltpu.VMEM((n_micro, t_loc, d_model), bf16),
            pltpu.VMEM((n_micro, t_loc, d_model), bf16),
            pltpu.VMEM((n_layers, 1, d_model), jnp.float32),
            pltpu.SemaphoreType.DMA((n_total + 1, 2)),
            pltpu.SemaphoreType.DMA((n_total + 1, 6)),
            pltpu.SemaphoreType.DMA((n_total + 1, 6)),
            pltpu.SemaphoreType.DMA((n_micro,)),
            pltpu.SemaphoreType.DMA((n_micro, n_blocks)),
            pltpu.SemaphoreType.DMA((n_micro, n_blocks)),
            pltpu.SemaphoreType.DMA((n_micro, n_blocks)),
            pltpu.SemaphoreType.DMA((n_micro, n_blocks)),
        ],
        compiler_params=pltpu.CompilerParams(collective_id=0, has_side_effects=True, vmem_limit_bytes=67043328),
    )(x_loc, lens, gain, w_kv, w_in, w_out)


def solution(mesh):
    act_spec = P(None, ("part", "data"), "model", None)
    def local_fn(x_blk, len_blk, gain_blk, w_in_blk, w_kv_blk, w_out_blk):
        n_micro, _, t_loc, d_model = x_blk.shape
        head_dim = w_kv_blk.shape[2] // 2
        out_rows = w_out_blk.shape[1]
        heads = (2 * out_rows - w_in_blk.shape[2]) // head_dim
        ff_head = out_rows // heads - head_dim
        n_chunks = heads // 2
        dims = (n_micro, gain_blk.shape[0], n_chunks, t_loc, d_model, head_dim, ff_head)
        y = run_kernel(x_blk.reshape(n_micro, t_loc, d_model), len_blk.reshape(n_micro), gain_blk, w_kv_blk, w_in_blk,
                       jnp.swapaxes(w_out_blk, 1, 2), dims)
        return y.reshape(x_blk.shape)

    return jax.shard_map(
        local_fn,
        mesh=mesh,
        in_specs=(act_spec, P(None, ("part", "data")), P(None, "data"), P(None, "data", "model"), P(None, "data", None), P(None, "model", "data")),
        out_specs=act_spec,
        check_vma=False,
    )
```

```python
import functools
import math

import jax
import jax.numpy as jnp
from jax import lax
from jax.experimental import pallas as pl
from jax.experimental.pallas import tpu as pltpu
from jax.sharding import PartitionSpec as P

MESH = pl.DeviceIdType.MESH
NORM_EPS = 1e-6
MASKED = -3e38
SIDE = 4
ROTATIONS = (("x", "y", "z"), ("y", "z", "x"), ("z", "x", "y"))
TILE = 256
BLOCK = 128
N_COMM = 99
BODY = True
DO_COMM = True
DO_COMPUTE = True
PLAN = (
        (("f", 0), (0, 0), (1, 0), (2, 0), ("f", 2), (0, 2), (1, 1), (2, 1), ("f", 4), (0, 3), (1, 2), (2, 2), ("f", 5), (0,
     4), (1, 3), (2, 3), (3, 0), (4, 0), ("CLEAR", 0), ("f", 6), ("GAIN", 0), ("N0", 0), ("N1", 0), (0, 5), (3, 1), (4, 1),
     (1, 4), ("K0", 0), ("K1", 0), (0, 6), (3, 2), (5, 0)),
        ((1, 5), (2, 4), (3, 3), (4, 2), (5, 1), (6, 0)),
        ((1, 6),),
        ((2, 5), (3, 4), (4, 3), (5, 2), (6, 1), (7, 0)),
        ((2, 6),),
        ((3, 5), (4, 4), (5, 3), (6, 2), (7, 1)),
        ((3, 6),),
        ((4, 5), (5, 4), (6, 3), (7, 2)),
        (("N0", 0), ("N1", 0), ("K0", 0), ("K1", 0), (4, 6)),
        ((5, 5), (6, 4), (7, 3)),
        ((5, 6),),
        ((6, 5), (7, 4)),
        ((6, 6),),
        ((7, 5),),
        ((7, 6),),
        (),
)


def mesh_kernel(dims, x_hbm, lens_ref, gain_ref, kv_ref, w_in_hbm, w_out_hbm, y_hbm,
                small, wsmall, wbig, xbuf, hbuf, kbuf, vbuf, acc, joined, zsend, zrecv, gain_buf,
                own_sem, wsend, wrecv, io_sem, hsend, hrecv, zs_sem, zr_sem):
    n_micro, n_layers, n_chunks, t_loc, d_model, head_dim, ff_head = dims
    n_total = n_layers * n_chunks
    pair_q, pair_f = 2 * head_dim, 2 * ff_head
    in_cols = pair_q + 2 * pair_f
    seq = 2 * t_loc
    me = lax.axis_index("data")
    core = lax.axis_index("model")
    pos = {"x": lax.rem(me, SIDE), "y": lax.rem(me // SIDE, SIDE), "z": me // (SIDE * SIDE)}
    stride = {"x": 1, "y": SIDE, "z": SIDE * SIDE}

    def shifted(axis, step):
        moved = lax.rem(pos[axis] + SIDE + step, SIDE)
        return moved, me + (moved - pos[axis]) * stride[axis]

    near = {(a, s): shifted(a, s) for a in "xyz" for s in (1, -1)}
    far = {a: shifted(a, 2) for a in "xyz"}
    sibling = {"model": 1 - core}

    barrier = pltpu.get_barrier_semaphore()
    for key in near:
        pl.semaphore_signal(barrier, inc=1, device_id={"data": near[key][1]}, device_id_type=MESH)
    for axis in "xyz":
        pl.semaphore_signal(barrier, inc=1, device_id={"data": far[axis][1]}, device_id_type=MESH)
    pl.semaphore_signal(barrier, inc=1, device_id=sibling, device_id_type=MESH)

    def load_x(m):
        return pltpu.make_async_copy(x_hbm.at[m], xbuf.at[m], io_sem.at[m])

    for m in range(n_micro):
        load_x(m).start()

    n_rows = kv_ref.shape[1]
    for layer in range(n_layers):
        small[:, layer * 128:(layer + 1) * 128] = kv_ref[layer]
    spread = (lax.rem(lax.broadcasted_iota(jnp.int32, (n_rows, 128), 1), n_rows)
              == lax.broadcasted_iota(jnp.int32, (n_rows, 128), 0)).astype(jnp.float32).astype(jnp.bfloat16)
    gains = jnp.dot(gain_ref[...], spread, preferred_element_type=jnp.float32)
    feature = lax.broadcasted_iota(jnp.int32, (n_rows, 128), 1) - n_rows * lax.rem(me, 128 // n_rows)
    row = lax.broadcasted_iota(jnp.int32, (n_rows, 128), 0)
    block = jnp.zeros((n_rows, 128), jnp.float32)
    for layer in range(n_layers):
        block = jnp.where(lax.rem(feature + layer, n_rows) == row, jnp.where(feature >= 0, jnp.where(
            feature < n_rows, gains[layer:layer + 1, :], block), block), block)
    small[:, n_layers * 128:] = block.astype(jnp.bfloat16)
    pl.semaphore_wait(barrier, 10)

    cut = 128 * ((in_cols // 128 + 1) // 2)
    out_cols = pair_q + pair_f
    big_parts = ((0, cut), (cut, in_cols), (in_cols, in_cols + out_cols))
    small_parts = ((0, 128), (128, 256), (256, 384))

    class Chunk:
        def __init__(self, buf, sources, parts, sem_idx, direct=(), turn=0):
            self.turn = turn
            self.buf, self.sources, self.parts, self.sem, self.direct = buf, sources, parts, sem_idx, direct

        def region(self, where, cols):
            return self.buf.at[where["z"], where["y"], where["x"], :, pl.ds(cols[0], cols[1] - cols[0])]

        def own(self):
            copies = []
            if self is first:
                return copies
            for j, (src, lo, hi) in enumerate(self.sources):
                dst = self.buf.at[pos["z"], pos["y"], pos["x"], :, pl.ds(lo, hi - lo)]
                copies.append(pltpu.make_async_copy(src, dst, own_sem.at[self.sem, j]))
            return copies

        def source(self, cols):
            for src, lo, hi in self.sources:
                if lo <= cols[0] and cols[1] <= hi:
                    return src.at[:, pl.ds(cols[0] - lo, cols[1] - cols[0])]

        def send(self, k):
            phase, second = k // 2, k % 2
            direct = phase in self.direct
            if direct and second:
                return
            for part, (lo, hi) in enumerate(self.parts):
                rot = ROTATIONS[(part + self.turn) % 3]
                axis = rot[phase]
                mid = lo + (((hi - lo) // 128 + 1) // 2) * 128
                for sign in (1, -1, 2)[:3 if direct else 2]:
                    where = {a: slice(None) for a in rot[:phase]}
                    where.update({a: pos[a] for a in rot[phase:]})
                    cols = (lo, hi)
                    if second:
                        where[axis] = near[axis, -sign][0]
                        if phase == 0:
                            cols = (lo, mid) if sign == 1 else (mid, hi)
                            if cols[0] == cols[1]:
                                continue
                        else:
                            where[rot[0]] = pl.ds(0, 2) if sign == 1 else pl.ds(2, 2)
                    dst = self.region(where, cols)
                    src = self.source(cols) if k == 0 else dst
                    pltpu.make_async_remote_copy(
                        src_ref=src, dst_ref=dst, send_sem=wsend.at[self.sem, k], recv_sem=wrecv.at[self.sem, k],
                        device_id={"data": far[axis][1] if sign == 2 else near[axis, sign][1]}, device_id_type=MESH).start()

        def bytes_of(self, k):
            count = 1 if k % 2 else 3 if k // 2 in self.direct else 2
            ref = (self.buf.at[0, 0, pl.ds(0, count)], self.buf.at[0, pl.ds(0, count)], self.buf.at[pl.ds(0, count)])[k // 2]
            return pltpu.make_async_remote_copy(
                src_ref=ref, dst_ref=ref, send_sem=wsend.at[self.sem, k], recv_sem=wrecv.at[self.sem, k],
                device_id={"data": near["x", 1][1]}, device_id_type=MESH)

        def step(self, k):
            if not DO_COMM:
                return
            if k == 0:
                for copy in self.own():
                    copy.start()
            elif k % 2 or k // 2 - 1 not in self.direct:
                self.bytes_of(k - 1).wait_recv()
            else:
                self.bytes_of(k - 2).wait_recv()
            if k == 2:
                for copy in self.own():
                    copy.wait()
            if k < 6:
                self.send(k)

        def finish(self):
            if not DO_COMM:
                return
            for k in range(6):
                if k % 2 == 0 or k // 2 not in self.direct:
                    self.bytes_of(k).wait_send()

    first = Chunk(wsmall, ((small, 0, 384),), small_parts, n_total, direct=(0, 1))

    def big(n):
        layer, c = n // n_chunks, n % n_chunks if isinstance(n, int) else lax.rem(n, n_chunks)

        def piece(ref, width):
            at = c * width if isinstance(c, int) else pl.multiple_of(c * width, 128)
            return ref.at[layer, :, pl.ds(at, width)]

        return Chunk(wbig.at[n], ((piece(w_in_hbm, in_cols), 0, in_cols),
                                  (piece(w_out_hbm, out_cols), in_cols, in_cols + out_cols)), big_parts, n,
                     direct=(0,) if isinstance(n, int) and n == 0 else (),
                     turn=n if isinstance(n, int) else 0)

    def step(n, k):
        if n < min(n_total, N_COMM):
            big(n).step(k)

    def store_y(m):
        return pltpu.make_async_copy(xbuf.at[m], y_hbm.at[m], io_sem.at[m])

    n_blocks = t_loc // BLOCK

    def send_h(m, r):
        rows = hbuf.at[m, pl.ds(pl.multiple_of(core * t_loc + r * BLOCK, BLOCK), BLOCK)]
        return pltpu.make_async_remote_copy(src_ref=rows, dst_ref=rows, send_sem=hsend.at[m, r], recv_sem=hrecv.at[m, r],
                                            device_id=sibling, device_id_type=MESH)

    def send_z(m, r):
        rows = pl.ds(pl.multiple_of(r * BLOCK, BLOCK), BLOCK)
        return pltpu.make_async_remote_copy(src_ref=zsend.at[m, rows], dst_ref=zrecv.at[m, rows], send_sem=zs_sem.at[m, r],
                                            recv_sem=zr_sem.at[m, r], device_id=sibling, device_id_type=MESH)

    def add_z(m, r):
        rows = pl.ds(pl.multiple_of(r * BLOCK, BLOCK), BLOCK)
        mine = pl.ds(pl.multiple_of(core * t_loc + r * BLOCK, BLOCK), BLOCK)
        send_z(m, r).wait_recv()
        z_own = acc[m, mine, :].astype(jnp.bfloat16).astype(jnp.float32)
        y = (xbuf[m, rows, :].astype(jnp.float32) + (z_own + zrecv[m, rows, :].astype(jnp.float32))).astype(jnp.bfloat16)
        xbuf[m, rows, :] = y
        acc[m, mine, :] = jnp.zeros((BLOCK, d_model), jnp.float32)
        send_z(m, r).wait_send()

    def norm(m, layer, after_z):
        def block_of(r, carry):
            if after_z:
                add_z(m, r)
            x_f32 = xbuf[m, pl.ds(pl.multiple_of(r * BLOCK, BLOCK), BLOCK), :].astype(jnp.float32)
            centered = x_f32 - jnp.mean(x_f32, axis=-1, keepdims=True)
            variance = jnp.mean(centered * centered, axis=-1, keepdims=True)
            h_act = (centered * lax.rsqrt(variance + NORM_EPS) * gain_buf[layer]).astype(jnp.bfloat16)
            hbuf[m, pl.ds(pl.multiple_of(core * t_loc + r * BLOCK, BLOCK), BLOCK), :] = h_act

            @pl.when(r > 0)
            def _():
                send_h(m, r - 1).start()
            return carry

        lax.fori_loop(0, n_blocks, block_of, 0)
        send_h(m, n_blocks - 1).start()

    def keys_values(m, layer):
        w_kv = wsmall[:, :, :, :, pl.ds(pl.multiple_of(layer * 128, 128), 128)].reshape(d_model, 2 * head_dim)
        lane = lax.broadcasted_iota(jnp.int32, (TILE, 2 * head_dim), 1)
        low = lane < head_dim
        length = lens_ref[m]

        def half(base):
            for t in range(t_loc // TILE):
                at = pl.multiple_of(base + t * TILE, TILE)
                rows = pl.ds(at, TILE)
                kv_f32 = jnp.dot(hbuf[m, rows, :], w_kv, preferred_element_type=jnp.float32)
                kv_f32 = kv_f32.astype(jnp.bfloat16).astype(jnp.float32)
                vk_f32 = pltpu.roll(kv_f32, head_dim, 1)
                key_pos = at + lax.broadcasted_iota(jnp.int32, (TILE, 2 * head_dim), 0)
                bias = jnp.where(key_pos < length, 0.0, MASKED)
                k_low = jnp.where(low, kv_f32, jnp.where(lane == head_dim, bias, 0.0))
                k_high = jnp.where(low, jnp.where(lane == 0, bias, 0.0), vk_f32)
                kbuf[m, 0, rows, :] = k_low.astype(jnp.bfloat16)
                kbuf[m, 1, rows, :] = k_high.astype(jnp.bfloat16)
                vbuf[m, 0, rows, :] = jnp.where(low, vk_f32, 0.0).astype(jnp.bfloat16)
                vbuf[m, 1, rows, :] = jnp.where(low, 0.0, kv_f32).astype(jnp.bfloat16)

        half(core * t_loc)
        for r in range(n_blocks):
            send_h(m, r).wait_recv()
        half((1 - core) * t_loc)
        for r in range(n_blocks):
            send_h(m, r).wait_send()

    exp_scale = (1.0 / math.sqrt(head_dim)) * math.log2(math.e)

    def body(n, m):
        lane = lax.broadcasted_iota(jnp.int32, (TILE, 2 * head_dim), 1)
        low = lane < head_dim
        seen = (lax.broadcasted_iota(jnp.int32, (TILE, TILE), 0) >= lax.broadcasted_iota(jnp.int32, (TILE, TILE), 1))
        w_in = wbig[n, :, :, :, :, :in_cols].reshape(d_model, in_cols)
        w_out = wbig[n, :, :, :, :, in_cols:].reshape(d_model, out_cols)
        one = jnp.ones((), jnp.bfloat16)
        zero = jnp.zeros((), jnp.bfloat16)
        unit = head_dim + 2 * ff_head
        n_tiles = seq // TILE
        proj, scores = {}, {}

        def rows(i):
            return slice(i * TILE, (i + 1) * TILE)

        def project(i):
            proj[i] = jnp.dot(hbuf[m, rows(i), :], w_in, preferred_element_type=jnp.float32).astype(jnp.bfloat16)

        def score(i):
            n_keys = (i + 1) * TILE
            at = unit - head_dim
            q_aug = (jnp.where(low, proj[i][:, :2 * head_dim], jnp.where(lane == head_dim, one, zero)),
                     jnp.where(low, jnp.where(lane == 0, one, zero), proj[i][:, at:at + 2 * head_dim]))
            for side in (0, 1):
                s = lax.dot_general(q_aug[side], kbuf[m, side, 0:n_keys, :], (((1,), (1,)), ((), ())),
                                    preferred_element_type=jnp.float32)
                diag = jnp.where(seen, s[:, n_keys - TILE:], MASKED)
                scores[i, side] = diag if i == 0 else jnp.concatenate([s[:, :n_keys - TILE], diag], axis=1)

        def softmax(s):
            top = jnp.max(s, axis=1, keepdims=True)
            e = jnp.exp2((s - top) * exp_scale)
            return (e * (1.0 / jnp.sum(e, axis=1, keepdims=True))).astype(jnp.bfloat16)

        def mlp(i, g_at, u_at, width):
            gate = proj[i][:, g_at:g_at + width].astype(jnp.float32)
            up = proj[i][:, u_at:u_at + width].astype(jnp.float32)
            half = 0.5 * gate
            return ((half + half * jnp.tanh(half)) * up).astype(jnp.bfloat16)

        def join(i):
            n_keys = (i + 1) * TILE
            probs = [softmax(scores.pop((i, side))) for side in (0, 1)]
            first = mlp(i, 0, ff_head, ff_head + 2 * head_dim)
            joined[rows(i), 2 * head_dim:ff_head] = first[:, 2 * head_dim:ff_head]
            joined[rows(i), ff_head + 2 * head_dim:] = mlp(i, unit + head_dim, unit + head_dim + ff_head, ff_head)
            outs = [jnp.dot(probs[side], vbuf[m, side, 0:n_keys, :], preferred_element_type=jnp.float32) for side in (0, 1)]
            pair = (outs[0] + outs[1]).astype(jnp.bfloat16)
            joined[rows(i), 0:2 * head_dim] = jnp.where(low, pair, first[:, :2 * head_dim])
            joined[rows(i), ff_head:ff_head + 2 * head_dim] = jnp.where(low, first[:, ff_head:], pair)

        def project_out(i):
            acc[m, rows(i), :] += lax.dot_general(joined[rows(i), :], w_out, (((1,), (1,)), ((), ())),
                                                  preferred_element_type=jnp.float32)

        order = list(range(n_tiles))[::-1]
        project(order[0])
        score(order[0])
        for at, i in enumerate(order):
            following = order[at + 1:at + 2]
            for j in following:
                project(j)
            join(i)
            for j in following:
                score(j)
            project_out(i)

    def stage_z(m):
        def block_of(r, carry):
            other = pl.ds(pl.multiple_of((1 - core) * t_loc + r * BLOCK, BLOCK), BLOCK)
            zsend[m, pl.ds(pl.multiple_of(r * BLOCK, BLOCK), BLOCK), :] = acc[m, other, :].astype(jnp.bfloat16)
            acc[m, other, :] = jnp.zeros((BLOCK, d_model), jnp.float32)

            @pl.when(r > 0)
            def _():
                send_z(m, r - 1).start()
            return carry

        lax.fori_loop(0, n_blocks, block_of, 0)
        send_z(m, n_blocks - 1).start()

    def clear_acc():
        def rows_of(r, carry):
            for m in range(n_micro):
                acc[m, pl.ds(pl.multiple_of(r * 64, 64), 64), :] = jnp.zeros((64, d_model), jnp.float32)
            return carry

        lax.fori_loop(0, seq // 64, rows_of, 0)

    def read_gains():
        table = wsmall[:, :, :, :, n_layers * 128:].astype(jnp.float32).reshape(d_model // 128, 128, 128)
        lane = lax.broadcasted_iota(jnp.int32, (128, 128), 1)
        row = lax.broadcasted_iota(jnp.int32, (128, 128), 0)
        for layer in range(n_layers):
            mine = lax.rem(lane + layer, n_rows) == lax.rem(row, n_rows)
            for k in range(d_model // 128):
                gain_buf[layer, :, k * 128:(k + 1) * 128] = jnp.sum(jnp.where(mine, table[k], 0.0), axis=0, keepdims=True)

    def run(event, layer):
        name, k = event
        if name == "f":
            first.step(k)
        elif not isinstance(name, str):
            step(name, k)
        elif DO_COMPUTE and name == "CLEAR":
            clear_acc()
        elif DO_COMPUTE and name == "GAIN":
            read_gains()
        elif name in ("N0", "N1"):
            m = int(name[1])
            if layer == 0:
                load_x(m).wait()
            if DO_COMPUTE:
                norm(m, layer, layer > 0)
        elif DO_COMPUTE:
            keys_values(int(name[1]), layer)

    if DO_COMM:
        wsmall[pos["z"], pos["y"], pos["x"]] = small[...]
    per_layer = n_chunks * n_micro
    for event in PLAN[0]:
        run(event, 0)

    def body_loop(it, carry):
        for at in range(1, len(PLAN)):
            if PLAN[at]:
                @pl.when(it == at)
                def _(at=at):
                    for event in PLAN[at]:
                        run(event, at // per_layer)

        if DO_COMPUTE:
            n, m = it // n_micro, lax.rem(it, n_micro)
            if BODY:
                body(n, m)

            @pl.when(lax.rem(it, per_layer) >= per_layer - n_micro)
            def _():
                stage_z(m)
        return carry

    lax.fori_loop(0, len(PLAN), body_loop, 0)
    for m in range(n_micro):
        if DO_COMPUTE:
            for r in range(n_blocks):
                add_z(m, r)
        store_y(m).start()
    first.finish()
    step_zero = big(0)
    if N_COMM > 0:
        step_zero.finish()

    def finish(n, carry):
        big(n).finish()
        return carry

    lax.fori_loop(1, min(n_total, N_COMM), finish, 0)
    for m in range(n_micro):
        store_y(m).wait()


def run_kernel(x_loc, lens, gain, w_kv, w_in, w_out, dims):
    n_micro, n_layers, n_chunks, t_loc, d_model, head_dim, ff_head = dims
    n_total = n_layers * n_chunks
    seq = 2 * t_loc
    any_spec = pl.BlockSpec(memory_space=pl.ANY)
    vmem_spec = pl.BlockSpec(memory_space=pltpu.VMEM)
    bf16 = jnp.bfloat16
    rows = w_in.shape[1]
    small_cols = (n_layers + 1) * 128
    n_blocks = t_loc // BLOCK
    return pl.pallas_call(
        functools.partial(mesh_kernel, dims),
        out_shape=jax.ShapeDtypeStruct((n_micro, t_loc, d_model), bf16),
        in_specs=[any_spec, pl.BlockSpec(memory_space=pltpu.SMEM), vmem_spec, vmem_spec, any_spec, any_spec],
        out_specs=any_spec,
        scratch_shapes=[
            pltpu.VMEM((rows, small_cols), bf16),
            pltpu.VMEM((SIDE, SIDE, SIDE, rows, small_cols), bf16),
            pltpu.VMEM((n_total, SIDE, SIDE, SIDE, w_in.shape[1], (w_in.shape[2] + w_out.shape[2]) // n_chunks), bf16),
            pltpu.VMEM((n_micro, t_loc, d_model), bf16),
            pltpu.VMEM((n_micro, seq, d_model), bf16),
            pltpu.VMEM((n_micro, 2, seq, 2 * head_dim), bf16),
            pltpu.VMEM((n_micro, 2, seq, 2 * head_dim), bf16),
            pltpu.VMEM((n_micro, seq, d_model), jnp.float32),
            pltpu.VMEM((seq, 2 * (head_dim + ff_head)), bf16),
            pltpu.VMEM((n_micro, t_loc, d_model), bf16),
            pltpu.VMEM((n_micro, t_loc, d_model), bf16),
            pltpu.VMEM((n_layers, 1, d_model), jnp.float32),
            pltpu.SemaphoreType.DMA((n_total + 1, 2)),
            pltpu.SemaphoreType.DMA((n_total + 1, 6)),
            pltpu.SemaphoreType.DMA((n_total + 1, 6)),
            pltpu.SemaphoreType.DMA((n_micro,)),
            pltpu.SemaphoreType.DMA((n_micro, n_blocks)),
            pltpu.SemaphoreType.DMA((n_micro, n_blocks)),
            pltpu.SemaphoreType.DMA((n_micro, n_blocks)),
            pltpu.SemaphoreType.DMA((n_micro, n_blocks)),
        ],
        compiler_params=pltpu.CompilerParams(collective_id=0, has_side_effects=True, vmem_limit_bytes=67043328),
    )(x_loc, lens, gain, w_kv, w_in, w_out)


def solution(mesh):
    act_spec = P(None, ("part", "data"), "model", None)
    def local_fn(x_blk, len_blk, gain_blk, w_in_blk, w_kv_blk, w_out_blk):
        n_micro, _, t_loc, d_model = x_blk.shape
        head_dim = w_kv_blk.shape[2] // 2
        out_rows = w_out_blk.shape[1]
        heads = (2 * out_rows - w_in_blk.shape[2]) // head_dim
        ff_head = out_rows // heads - head_dim
        n_chunks = heads // 2
        dims = (n_micro, gain_blk.shape[0], n_chunks, t_loc, d_model, head_dim, ff_head)
        y = run_kernel(x_blk.reshape(n_micro, t_loc, d_model), len_blk.reshape(n_micro), gain_blk, w_kv_blk, w_in_blk,
                       jnp.swapaxes(w_out_blk, 1, 2), dims)
        return y.reshape(x_blk.shape)

    return jax.shard_map(
        local_fn,
        mesh=mesh,
        in_specs=(act_spec, P(None, ("part", "data")), P(None, "data"), P(None, "data", "model"), P(None, "data", None), P(None, "model", "data")),
        out_specs=act_spec,
        check_vma=False,
    )
```
